256 devices in a mesh: dp: 16 (over z, core), mp: 16 (over y, x).
Axes of the slice: x: 4, y: 4, z: 8, core: 2. Of those that a mesh axis runs over, the one named last changes fastest.
Arguments:
- inputs: bfloat16 [4096, 8192], P('dp', 'mp'), may hold values from -6 to 6
- out_grads: bfloat16 [4096, 8192], P('dp', 'mp'), may hold values from -6 to 6
- left_old: float32 [8192, 8192], P('dp', 'mp'), may hold values from -2 to 4, as said below
- right_old: float32 [8192, 8192], P('dp', 'mp'), may hold values from -2 to 4, as said below
- left_roots: float32 [8192, 8192], P('dp', 'mp'), may hold values from -2 to 4, as said below
- right_roots: float32 [8192, 8192], P('dp', 'mp'), may hold values from -2 to 4, as said below
- ages: int32 [16, 16], replicated, may hold values from 0 to 199, as said below
Outputs:
- precond: float32 [8192, 8192], P('dp', 'mp')
- left_new: float32 [8192, 8192], P('dp', 'mp')
- right_new: float32 [8192, 8192], P('dp', 'mp')
The draws below stay inside these ranges and needn't reach their ends.
Inputs may be any that keep to these rules, and one draw needn't show every extreme that they name: `ages`: in every row i, blocks (i, j) and (i, j + 8) are never both due, and every row has a due block. `left_old`: every 512 x 512 block is symmetric and positive definite. `right_old`: every 512 x 512 block is symmetric and positive definite. `left_roots`: every 512 x 512 block is symmetric and positive definite. `right_roots`: every 512 x 512 block is symmetric and positive definite.
All inputs are finite; a program needn't handle non-finite values.
Results may differ from the reference program's by a relative error of at most 0.001.
Values may be sent and summed in bfloat16 or wider, within the bound.
A program may use at most 128 MiB of HBM per device.

```python
import jax
import jax.numpy as jnp
from jax import lax

BS = 512
ITERS = 3
PERIOD = 100
D_IN = 8192
D_OUT = 8192
TOKENS = 4096


def definite_blocks(key, spread, shift):
    rows_blocks = D_IN // BS
    cols_blocks = D_OUT // BS
    base = jax.random.normal(key, (rows_blocks, cols_blocks, BS, BS), jnp.float32)
    gram = jnp.einsum('abij,abkj->abik', base, base) / BS
    stack = spread * gram + shift * jnp.eye(BS, dtype=jnp.float32)
    return stack.transpose(0, 2, 1, 3).reshape(rows_blocks * BS, cols_blocks * BS)


def draw_left_old(key, part):
    return definite_blocks(jax.random.fold_in(key, 11), 1.0, 0.5)


def draw_right_old(key, part):
    return definite_blocks(jax.random.fold_in(key, 12), 1.0, 0.5)


def draw_left_roots(key, part):
    return definite_blocks(jax.random.fold_in(key, 13), 0.5, 0.5)


def draw_right_roots(key, part):
    return definite_blocks(jax.random.fold_in(key, 14), 0.5, 0.5)


def draw_ages(key, part):
    rows_blocks = D_IN // BS
    half_cols = D_OUT // BS // 2
    state = jax.random.randint(jax.random.fold_in(key, 21), (rows_blocks, half_cols), 0, 3)
    forced_col = jax.random.randint(jax.random.fold_in(key, 22), (rows_blocks, 1), 0, half_cols)
    forced_side = jax.random.randint(jax.random.fold_in(key, 23), (rows_blocks, 1), 1, 3)
    column_ids = jnp.arange(half_cols, dtype=jnp.int32)[None, :]
    state = jnp.where(column_ids == forced_col, forced_side, state)
    due_first = jax.random.randint(jax.random.fold_in(key, 24), (rows_blocks, half_cols), PERIOD, 2 * PERIOD)
    due_second = jax.random.randint(jax.random.fold_in(key, 25), (rows_blocks, half_cols), PERIOD, 2 * PERIOD)
    wait_first = jax.random.randint(jax.random.fold_in(key, 26), (rows_blocks, half_cols), 0, PERIOD)
    wait_second = jax.random.randint(jax.random.fold_in(key, 27), (rows_blocks, half_cols), 0, PERIOD)
    first_half = jnp.where(state == 1, due_first, wait_first)
    second_half = jnp.where(state == 2, due_second, wait_second)
    return jnp.concatenate([first_half, second_half], axis=1).astype(jnp.int32)


def levels(stream_key, extent, pieces, least, largest):
    def one(position, blocks):
        draws = jax.random.uniform(jax.random.fold_in(jax.random.fold_in(stream_key, 6), position), (blocks,), jnp.float32, least / len(pieces), largest / len(pieces))
        return jnp.repeat(jnp.exp(draws), extent[position] // blocks).reshape((-1,) + (1,) * (len(extent) - position - 1))

    factor_of = one(*pieces[0])
    for cut in pieces[1:]:
        factor_of = factor_of * one(*cut)
    return factor_of


def scatter_about(own_key, dims, deviation, bound, pieces=(), kind=jnp.bfloat16):
    drawn = deviation * jax.random.normal(own_key, dims, jnp.float32)
    if pieces:
        drawn = drawn * levels(own_key, dims, pieces, -0.22, 0.18)
    return jnp.clip(drawn, -bound, bound).astype(kind)


def setup_inputs(seed: int = 0) -> dict:
    seeds = jax.random.split(jax.random.key(seed), 8)
    inputs = scatter_about(seeds[0], (TOKENS, D_IN), 1.0, 6.0, ((0, 16), (1, 16)))
    out_grads = scatter_about(seeds[1], (TOKENS, D_OUT), 1.0, 6.0, ((0, 16), (1, 16)))
    left_old = draw_left_old(jax.random.fold_in(seeds[7], 71), 0)
    right_old = draw_right_old(jax.random.fold_in(seeds[7], 71), 0)
    left_roots = draw_left_roots(jax.random.fold_in(seeds[7], 71), 0)
    right_roots = draw_right_roots(jax.random.fold_in(seeds[7], 71), 0)
    ages = draw_ages(jax.random.fold_in(seeds[7], 71), 0)
    return {"inputs": inputs, "out_grads": out_grads, "left_old": left_old, "right_old": right_old, "left_roots": left_roots, "right_roots": right_roots, "ages": ages}


decay_rate = 0.95
ridge = 0.001

def product(first, second):
    return jnp.dot(first, second, precision=lax.Precision.HIGHEST, preferred_element_type=jnp.float32)

def gram_rows(matrix):
    return lax.dot_general(matrix, matrix, (((1,), (1,)), ((), ())), precision=lax.Precision.HIGHEST, preferred_element_type=jnp.float32)

def gram_cols(matrix):
    return lax.dot_general(matrix, matrix, (((0,), (0,)), ((), ())), precision=lax.Precision.HIGHEST, preferred_element_type=jnp.float32)

def inverse_root(stat):
    block_order = stat.shape[0]
    identity = jnp.eye(block_order, dtype=jnp.float32)
    matrix = stat + ridge * identity
    norm_scale = jnp.sqrt(jnp.sum(matrix * matrix) / block_order + 1e-06)
    moment = matrix / norm_scale
    inverse = identity
    for iteration in range(ITERS):
        factor = (5.0 * identity - moment) / 4.0
        if iteration == 0:
            inverse = factor * norm_scale ** (-0.25)
        else:
            inverse = product(inverse, factor)
        if iteration + 1 < ITERS:
            square = product(factor, factor)
            moment = product(product(square, square), moment)
    return inverse

def reference(inputs, out_grads, left_old, right_old, left_roots, right_roots, ages):
    gradient = lax.dot_general(inputs.astype(jnp.float32), out_grads.astype(jnp.float32), (((0,), (0,)), ((), ())), precision=lax.Precision.HIGHEST, preferred_element_type=jnp.float32) * TOKENS ** (-0.5)
    rows_blocks = D_IN // BS
    cols_blocks = D_OUT // BS

    def to_blocks(whole):
        return whole.reshape(rows_blocks, BS, cols_blocks, BS).transpose(0, 2, 1, 3).reshape(rows_blocks * cols_blocks, BS, BS)

    def from_blocks(stack):
        return stack.reshape(rows_blocks, cols_blocks, BS, BS).transpose(0, 2, 1, 3).reshape(D_IN, D_OUT)
    refresh = (ages >= PERIOD).reshape(-1)

    def per_block(items):
        block_grad, left_prev, right_prev, left_inv_old, right_inv_old, refresh_due = items
        left_stat = decay_rate * left_prev + gram_rows(block_grad) / BS
        right_stat = decay_rate * right_prev + gram_cols(block_grad) / BS
        left_inv = lax.cond(refresh_due, lambda: inverse_root(left_stat), lambda: left_inv_old)
        right_inv = lax.cond(refresh_due, lambda: inverse_root(right_stat), lambda: right_inv_old)
        return (product(product(left_inv, block_grad), right_inv), left_stat, right_stat)
    precond, left_new, right_new = lax.map(per_block, (to_blocks(gradient), to_blocks(left_old), to_blocks(right_old), to_blocks(left_roots), to_blocks(right_roots), refresh))
    return (from_blocks(precond), from_blocks(left_new), from_blocks(right_new))
```

```python
import jax
import jax.numpy as jnp
from jax import lax
from jax.experimental import pallas as pl
from jax.experimental.pallas import tpu as pltpu
from jax.sharding import PartitionSpec as P

ITERS = 3
PERIOD = 100
NZ, NY, NX = 8, 4, 4
PARTS = 16
MESH = pl.DeviceIdType.MESH

decay_rate = 0.95
ridge = 0.001


def gather_kernel(
    scale, a_hbm, b_hbm, g_ref, abuf, bbuf, load_sem, t_send, t_recv, a_send, a_recv, b_send, b_recv
):
    rows = a_hbm.shape[0]
    half, quarter = rows // 2, rows // 4
    i = lax.axis_index("dp")
    k = lax.axis_index("mp")
    z, c = i // 2, i % 2
    y, x = k // NX, k % NX

    def place(dz=0, dy=0, dx=0, other=False):
        core = 1 - c if other else c
        return {
            "dp": ((z + dz + NZ) % NZ) * 2 + core,
            "mp": ((y + dy + NY) % NY) * NX + (x + dx + NX) % NX,
        }

    target = {"dp": k, "mp": (i + k) % PARTS}
    origin = {"dp": (k - i + PARTS) % PARTS, "mp": i}
    own_a = (k - i + PARTS) % PARTS
    is_self = (i == 0) & (k == 0)

    neighbours = [
        place(dz=1), place(dz=-1), place(dy=1), place(dy=-1),
        place(dx=1), place(dx=-1), place(other=True),
    ]

    load = pltpu.make_async_copy(b_hbm, bbuf.at[i], load_sem.at[0])
    load.start()
    barrier = pltpu.get_barrier_semaphore()
    for device in neighbours + [origin]:
        pl.semaphore_signal(barrier, inc=1, device_id=device, device_id_type=MESH)
    pl.semaphore_wait(barrier, len(neighbours) + 1)

    pending = []

    def entry(part):
        rows_of = pl.ds(part * half, half)
        return pltpu.make_async_remote_copy(
            src_ref=a_hbm.at[rows_of],
            dst_ref=abuf.at[i, rows_of],
            send_sem=t_send.at[part],
            recv_sem=t_recv.at[part],
            device_id=target,
            device_id_type=MESH,
        )

    def entry_arrival(part):
        rows_of = pl.ds(part * half, half)
        return pltpu.make_async_remote_copy(
            src_ref=a_hbm.at[rows_of],
            dst_ref=abuf.at[own_a, rows_of],
            send_sem=t_send.at[part],
            recv_sem=t_recv.at[part],
            device_id=target,
            device_id_type=MESH,
        )

    def entry_local(part):
        rows_of = pl.ds(part * half, half)
        return pltpu.make_async_copy(
            a_hbm.at[rows_of], abuf.at[own_a, rows_of], t_recv.at[part]
        )

    for part in range(2):

        @pl.when(is_self)
        def _():
            entry_local(part).start()

        @pl.when(jnp.logical_not(is_self))
        def _():
            entry(part).start()

    def a_copy(slot, first, count, index, sem, device):
        window = abuf.at[slot, pl.ds(first, count)]
        return pltpu.make_async_remote_copy(
            src_ref=window,
            dst_ref=window,
            send_sem=a_send.at[index],
            recv_sem=a_recv.at[slot, sem],
            device_id=device,
            device_id_type=MESH,
        )

    def b_copy(slot, first, count, index, sem, device):
        window = bbuf.at[slot, pl.ds(first, count)]
        return pltpu.make_async_remote_copy(
            src_ref=window,
            dst_ref=window,
            send_sem=b_send.at[index],
            recv_sem=b_recv.at[slot, sem],
            device_id=device,
            device_id_type=MESH,
        )

    counts = {"a": 0, "b": 0}

    def send(kind, slot, first, count, sem, device):
        make = a_copy if kind == "a" else b_copy
        copy = make(slot, first, count, counts[kind], sem, device)
        counts[kind] += 1
        copy.start()
        pending.append(copy)

    def arrive(kind, slot, first, count, sem):
        make = a_copy if kind == "a" else b_copy
        make(slot, first, count, 0, sem, place(dx=1)).wait_recv()

    def z_slot(distance):
        return ((z + distance + NZ) % NZ) * 2 + c

    load.wait()
    for part in range(2):
        for step in (1, -1):
            send("b", i, part * half, half, part, place(dz=step))
    send("b", i, 0, rows, 0, place(other=True))

    def ring(distance, part):
        for step in (1, -1):
            slot = z_slot(-step * distance)
            if distance < 4:
                arrive("b", slot, part * half, half, part)
                if distance < 3 or part == (0 if step == 1 else 1):
                    send("b", slot, part * half, half, part, place(dz=step))
                if part == 1:
                    send("b", slot, 0, rows, 0, place(other=True))

    def a_slot(h, p, s):
        dx, dy = (p, s) if h == 0 else (s, p)
        where = ((y + dy + NY) % NY) * NX + (x + dx + NX) % NX
        return (where - i + PARTS) % PARTS

    def primary(h, step):
        return place(dx=step) if h == 0 else place(dy=step)

    def secondary(h, step):
        return place(dy=step) if h == 0 else place(dx=step)

    def send_half(h, slot, device):
        send("a", slot, h * half, half, 2 * h, device)

    def send_quarter(h, slot, step, device):
        q = 2 * h + (0 if step == 1 else 1)
        send("a", slot, q * quarter, quarter, q, device)

    def arrive_half(h, slot):
        arrive("a", slot, h * half, half, 2 * h)

    def arrive_quarters(h, slot):
        for q in (2 * h, 2 * h + 1):
            arrive("a", slot, q * quarter, quarter, q)

    def first_step():
        for h in range(2):

            @pl.when(is_self)
            def _():
                entry_local(h).wait()

            @pl.when(jnp.logical_not(is_self))
            def _():
                entry_arrival(h).wait_recv()

            for step in (1, -1):
                send_half(h, a_slot(h, 0, 0), primary(h, step))
            for step in (1, -1):
                send_half(h, a_slot(h, 0, 0), secondary(h, step))

    def primary_near():
        for h in range(2):
            for step in (1, -1):
                slot = a_slot(h, -step, 0)
                arrive_half(h, slot)
                send_quarter(h, slot, step, primary(h, step))
                for side in (1, -1):
                    send_half(h, slot, secondary(h, side))

    def primary_far():
        for h in range(2):
            slot = a_slot(h, 2, 0)
            arrive_quarters(h, slot)
            for side in (1, -1):
                send_half(h, slot, secondary(h, side))

    def secondary_near(p):
        for h in range(2):
            for step in (1, -1):
                slot = a_slot(h, p, -step)
                arrive_half(h, slot)
                send_quarter(h, slot, step, secondary(h, step))

    first_step()
    ring(1, 0)
    primary_near()
    ring(1, 1)
    secondary_near(0)
    ring(2, 0)
    primary_far()
    ring(2, 1)
    secondary_near(-1)
    ring(3, 0)
    secondary_near(1)
    ring(3, 1)
    secondary_near(2)
    far = z_slot(4)
    for part in range(2):
        arrive("b", far, part * half, half, part)
    send("b", far, 0, rows, 0, place(other=True))
    for h in range(2):
        for p in (0, -1, 1, 2):
            arrive_quarters(h, a_slot(h, p, 2))
    for distance in range(NZ):
        arrive("b", ((z + distance) % NZ) * 2 + 1 - c, 0, rows, 0)

    width = a_hbm.shape[1]
    tile = 256
    for m in range(width // tile):
        first = abuf[:, :, m * tile : (m + 1) * tile].reshape(PARTS * rows, tile)
        second = bbuf[...].reshape(PARTS * rows, b_hbm.shape[1])
        g_ref[m * tile : (m + 1) * tile, :] = scale * lax.dot_general(
            first, second, (((0,), (0,)), ((), ())), preferred_element_type=jnp.float32
        )

    for copy in pending:
        copy.wait_send()

    @pl.when(jnp.logical_not(is_self))
    def _():
        for part in range(2):
            entry(part).wait_send()


def gather_product(inputs, out_grads, scale):
    rows, width = inputs.shape
    columns = out_grads.shape[1]
    return pl.pallas_call(
        lambda *refs: gather_kernel(scale, *refs),
        out_shape=jax.ShapeDtypeStruct((width, columns), jnp.float32),
        in_specs=[pl.BlockSpec(memory_space=pl.ANY)] * 2,
        out_specs=pl.BlockSpec(memory_space=pltpu.VMEM),
        scratch_shapes=[
            pltpu.VMEM((PARTS, rows, width), jnp.bfloat16),
            pltpu.VMEM((PARTS, rows, columns), jnp.bfloat16),
            pltpu.SemaphoreType.DMA((1,)),
            pltpu.SemaphoreType.DMA((2,)),
            pltpu.SemaphoreType.DMA((2,)),
            pltpu.SemaphoreType.DMA((40,)),
            pltpu.SemaphoreType.DMA((PARTS, 4)),
            pltpu.SemaphoreType.DMA((32,)),
            pltpu.SemaphoreType.DMA((PARTS, 2)),
        ],
        compiler_params=pltpu.CompilerParams(collective_id=0, has_side_effects=True),
        name="gather_product",
    )(inputs, out_grads)


def product(first, second):
    return jnp.dot(
        first, second, precision=lax.Precision.HIGH, preferred_element_type=jnp.float32
    )


def gram_rows(matrix):
    return lax.dot_general(
        matrix,
        matrix,
        (((1,), (1,)), ((), ())),
        precision=lax.Precision.HIGH,
        preferred_element_type=jnp.float32,
    )


def gram_cols(matrix):
    return lax.dot_general(
        matrix,
        matrix,
        (((0,), (0,)), ((), ())),
        precision=lax.Precision.HIGH,
        preferred_element_type=jnp.float32,
    )


def inverse_root(stat):
    block_order = stat.shape[0]
    identity = jnp.eye(block_order, dtype=jnp.float32)
    matrix = stat + ridge * identity
    norm_scale = jnp.sqrt(jnp.sum(matrix * matrix) / block_order + 1e-06)
    moment = matrix / norm_scale
    inverse = identity
    for iteration in range(ITERS):
        factor = (5.0 * identity - moment) / 4.0
        if iteration == 0:
            inverse = factor * norm_scale ** (-0.25)
        else:
            inverse = product(inverse, factor)
        if iteration + 1 < ITERS:
            square = product(factor, factor)
            moment = product(product(square, square), moment)
    return inverse


def shards(inputs, out_grads, left_old, right_old, left_roots, right_roots, ages):
    block_order = left_old.shape[0]
    tokens_all = out_grads.shape[0] * lax.axis_size("dp")
    gradient = gather_product(inputs, out_grads, tokens_all ** (-0.5))
    left_stat = decay_rate * left_old + gram_rows(gradient) / block_order
    right_stat = decay_rate * right_old + gram_cols(gradient) / block_order
    row_index = lax.axis_index("dp")
    col_index = lax.axis_index("mp")
    own_due = ages[row_index, col_index] >= PERIOD
    left_inv = lax.cond(own_due, lambda: inverse_root(left_stat), lambda: left_roots)
    right_inv = lax.cond(own_due, lambda: inverse_root(right_stat), lambda: right_roots)
    precond = product(product(left_inv, gradient), right_inv)
    return (precond, left_stat, right_stat)


def solution(mesh):
    in_specs = (
        P("dp", "mp"),
        P("dp", "mp"),
        P("dp", "mp"),
        P("dp", "mp"),
        P("dp", "mp"),
        P("dp", "mp"),
        P(),
    )
    out_specs = (P("dp", "mp"), P("dp", "mp"), P("dp", "mp"))
    return jax.shard_map(shards, mesh=mesh, in_specs=in_specs, out_specs=out_specs, check_vma=False)
```

```python
import jax
import jax.numpy as jnp
from jax import lax
from jax.experimental import pallas as pl
from jax.experimental.pallas import tpu as pltpu
from jax.sharding import PartitionSpec as P

ITERS = 3
PERIOD = 100
NZ, NY, NX = 8, 4, 4
PARTS = 16
MESH = pl.DeviceIdType.MESH

decay_rate = 0.95
ridge = 0.001


def gather_kernel(
    scale, a_hbm, b_hbm, g_ref, abuf, bbuf, load_sem, t_send, t_recv, a_send, a_recv, b_send, b_recv
):
    rows = a_hbm.shape[0]
    half, quarter = rows // 2, rows // 4
    i = lax.axis_index("dp")
    k = lax.axis_index("mp")
    z, c = i // 2, i % 2
    y, x = k // NX, k % NX

    def place(dz=0, dy=0, dx=0, other=False):
        core = 1 - c if other else c
        return {
            "dp": ((z + dz + NZ) % NZ) * 2 + core,
            "mp": ((y + dy + NY) % NY) * NX + (x + dx + NX) % NX,
        }

    target = {"dp": k, "mp": (i + k) % PARTS}
    origin = {"dp": (k - i + PARTS) % PARTS, "mp": i}
    own_a = (k - i + PARTS) % PARTS
    is_self = (i == 0) & (k == 0)

    neighbours = [
        place(dz=1), place(dz=-1), place(dy=1), place(dy=-1),
        place(dx=1), place(dx=-1), place(other=True),
    ]

    load = pltpu.make_async_copy(b_hbm, bbuf.at[i], load_sem.at[0])
    load.start()
    barrier = pltpu.get_barrier_semaphore()
    for device in neighbours + [origin]:
        pl.semaphore_signal(barrier, inc=1, device_id=device, device_id_type=MESH)
    pl.semaphore_wait(barrier, len(neighbours) + 1)

    pending = []

    def entry(part):
        rows_of = pl.ds(part * half, half)
        return pltpu.make_async_remote_copy(
            src_ref=a_hbm.at[rows_of],
            dst_ref=abuf.at[i, rows_of],
            send_sem=t_send.at[part],
            recv_sem=t_recv.at[part],
            device_id=target,
            device_id_type=MESH,
        )

    def entry_arrival(part):
        rows_of = pl.ds(part * half, half)
        return pltpu.make_async_remote_copy(
            src_ref=a_hbm.at[rows_of],
            dst_ref=abuf.at[own_a, rows_of],
            send_sem=t_send.at[part],
            recv_sem=t_recv.at[part],
            device_id=target,
            device_id_type=MESH,
        )

    def entry_local(part):
        rows_of = pl.ds(part * half, half)
        return pltpu.make_async_copy(
            a_hbm.at[rows_of], abuf.at[own_a, rows_of], t_recv.at[part]
        )

    for part in range(2):

        @pl.when(is_self)
        def _():
            entry_local(part).start()

        @pl.when(jnp.logical_not(is_self))
        def _():
            entry(part).start()

    def a_copy(slot, first, count, index, sem, device):
        window = abuf.at[slot, pl.ds(first, count)]
        return pltpu.make_async_remote_copy(
            src_ref=window,
            dst_ref=window,
            send_sem=a_send.at[index],
            recv_sem=a_recv.at[slot, sem],
            device_id=device,
            device_id_type=MESH,
        )

    def b_copy(slot, first, count, index, sem, device):
        window = bbuf.at[slot, pl.ds(first, count)]
        return pltpu.make_async_remote_copy(
            src_ref=window,
            dst_ref=window,
            send_sem=b_send.at[index],
            recv_sem=b_recv.at[slot, sem],
            device_id=device,
            device_id_type=MESH,
        )

    counts = {"a": 0, "b": 0}

    def send(kind, slot, first, count, sem, device):
        make = a_copy if kind == "a" else b_copy
        copy = make(slot, first, count, counts[kind], sem, device)
        counts[kind] += 1
        copy.start()
        pending.append(copy)

    def arrive(kind, slot, first, count, sem):
        make = a_copy if kind == "a" else b_copy
        make(slot, first, count, 0, sem, place(dx=1)).wait_recv()

    def z_slot(distance):
        return ((z + distance + NZ) % NZ) * 2 + c

    load.wait()
    for part in range(2):
        for step in (1, -1):
            send("b", i, part * half, half, part, place(dz=step))
    send("b", i, 0, rows, 0, place(other=True))

    def ring(distance, part):
        for step in (1, -1):
            slot = z_slot(-step * distance)
            if distance < 4:
                arrive("b", slot, part * half, half, part)
                if distance < 3 or part == (0 if step == 1 else 1):
                    send("b", slot, part * half, half, part, place(dz=step))
                if part == 1:
                    send("b", slot, 0, rows, 0, place(other=True))

    def a_slot(h, p, s):
        dx, dy = (p, s) if h == 0 else (s, p)
        where = ((y + dy + NY) % NY) * NX + (x + dx + NX) % NX
        return (where - i + PARTS) % PARTS

    def primary(h, step):
        return place(dx=step) if h == 0 else place(dy=step)

    def secondary(h, step):
        return place(dy=step) if h == 0 else place(dx=step)

    def send_half(h, slot, device):
        send("a", slot, h * half, half, 2 * h, device)

    def send_quarter(h, slot, step, device):
        q = 2 * h + (0 if step == 1 else 1)
        send("a", slot, q * quarter, quarter, q, device)

    def arrive_half(h, slot):
        arrive("a", slot, h * half, half, 2 * h)

    def arrive_quarters(h, slot):
        for q in (2 * h, 2 * h + 1):
            arrive("a", slot, q * quarter, quarter, q)

    def first_step():
        for h in range(2):

            @pl.when(is_self)
            def _():
                entry_local(h).wait()

            @pl.when(jnp.logical_not(is_self))
            def _():
                entry_arrival(h).wait_recv()

            for step in (1, -1):
                send_half(h, a_slot(h, 0, 0), primary(h, step))
            for step in (1, -1):
                send_half(h, a_slot(h, 0, 0), secondary(h, step))

    def primary_near():
        for h in range(2):
            for step in (1, -1):
                slot = a_slot(h, -step, 0)
                arrive_half(h, slot)
                send_quarter(h, slot, step, primary(h, step))
                for side in (1, -1):
                    send_half(h, slot, secondary(h, side))

    def primary_far():
        for h in range(2):
            slot = a_slot(h, 2, 0)
            arrive_quarters(h, slot)
            for side in (1, -1):
                send_half(h, slot, secondary(h, side))

    def secondary_near(p):
        for h in range(2):
            for step in (1, -1):
                slot = a_slot(h, p, -step)
                arrive_half(h, slot)
                send_quarter(h, slot, step, secondary(h, step))

    first_step()
    ring(1, 0)
    primary_near()
    ring(1, 1)
    secondary_near(0)
    ring(2, 0)
    primary_far()
    ring(2, 1)
    secondary_near(-1)
    ring(3, 0)
    secondary_near(1)
    ring(3, 1)
    secondary_near(2)
    far = z_slot(4)
    for part in range(2):
        arrive("b", far, part * half, half, part)
    send("b", far, 0, rows, 0, place(other=True))
    for h in range(2):
        for p in (0, -1, 1, 2):
            arrive_quarters(h, a_slot(h, p, 2))
    for distance in range(NZ):
        arrive("b", ((z + distance) % NZ) * 2 + 1 - c, 0, rows, 0)

    width = a_hbm.shape[1]
    tile = 256
    for m in range(width // tile):
        first = abuf[:, :, m * tile : (m + 1) * tile].reshape(PARTS * rows, tile)
        second = bbuf[...].reshape(PARTS * rows, b_hbm.shape[1])
        g_ref[m * tile : (m + 1) * tile, :] = scale * lax.dot_general(
            first, second, (((0,), (0,)), ((), ())), preferred_element_type=jnp.float32
        )

    for copy in pending:
        copy.wait_send()

    @pl.when(jnp.logical_not(is_self))
    def _():
        for part in range(2):
            entry(part).wait_send()


def gather_product(inputs, out_grads, scale):
    rows, width = inputs.shape
    columns = out_grads.shape[1]
    return pl.pallas_call(
        lambda *refs: gather_kernel(scale, *refs),
        out_shape=jax.ShapeDtypeStruct((width, columns), jnp.float32),
        in_specs=[pl.BlockSpec(memory_space=pl.ANY)] * 2,
        out_specs=pl.BlockSpec(memory_space=pltpu.VMEM),
        scratch_shapes=[
            pltpu.VMEM((PARTS, rows, width), jnp.bfloat16),
            pltpu.VMEM((PARTS, rows, columns), jnp.bfloat16),
            pltpu.SemaphoreType.DMA((1,)),
            pltpu.SemaphoreType.DMA((2,)),
            pltpu.SemaphoreType.DMA((2,)),
            pltpu.SemaphoreType.DMA((40,)),
            pltpu.SemaphoreType.DMA((PARTS, 4)),
            pltpu.SemaphoreType.DMA((32,)),
            pltpu.SemaphoreType.DMA((PARTS, 2)),
        ],
        compiler_params=pltpu.CompilerParams(collective_id=0, has_side_effects=True),
        name="gather_product",
    )(inputs, out_grads)


def split(value):
    high = value.astype(jnp.bfloat16)
    return high, (value - high.astype(jnp.float32)).astype(jnp.bfloat16)


def dot(first, second):
    return jnp.dot(first, second, preferred_element_type=jnp.float32)


SLOTS = 21
G, GT, T = 18, 19, 20
M0, F1, S, Q, M1, F2, X2, F3, X3 = range(9)
TILE = 256


def roots_kernel(
    ages, g_ref, left_old, right_old, left_roots, right_roots,
    precond, left_new, right_new, old, new, high, low, load_sem, store_sem, roots_sem,
):
    order = g_ref.shape[0]
    due = ages[lax.axis_index("dp"), lax.axis_index("mp")] >= PERIOD
    loads = [
        pltpu.make_async_copy(source, old.at[side], load_sem.at[side])
        for side, source in enumerate((left_old, right_old))
    ]
    for load in loads:
        load.start()
    tiles = range(order // TILE)

    def columns(tile):
        return pl.ds(tile * TILE, TILE)

    def eye(tile):
        rows = lax.broadcasted_iota(jnp.int32, (order, TILE), 0)
        return rows == lax.broadcasted_iota(jnp.int32, (order, TILE), 1) + tile * TILE

    def put(slot, tile, value):
        high[slot, :, columns(tile)], low[slot, :, columns(tile)] = split(value)

    def multiply(first, second, tile):
        right_high = high[second, :, columns(tile)]
        return (
            dot(high[first], right_high)
            + dot(high[first], low[second, :, columns(tile)])
            + dot(low[first], right_high)
        )

    for tile in tiles:
        part = g_ref[:, columns(tile)]
        put(G, tile, part)
        rows = pl.ds(tile * TILE, TILE)
        high[GT, rows, :], low[GT, rows, :] = split(part.T)

    stores = []
    squares = []
    for side, (first, second, out) in enumerate(((G, GT, left_new), (GT, G, right_new))):
        loads[side].wait()
        total = 0.0
        for tile in tiles:
            stat = decay_rate * old[side, :, columns(tile)] + multiply(first, second, tile) * (
                1.0 / order
            )
            new[side, :, columns(tile)] = stat
            ridged = jnp.where(eye(tile), stat + ridge, stat)
            total = total + jnp.sum(ridged * ridged)
        squares.append(total)
        store = pltpu.make_async_copy(new.at[side], out, store_sem.at[side])
        store.start()
        stores.append(store)

    def next_factor(slot, tile, moment):
        put(slot, tile, jnp.where(eye(tile), 1.25 - 0.25 * moment, -0.25 * moment))

    @pl.when(due)
    def _():
        scales = []
        for side in range(2):
            base = 9 * side
            scale = jnp.sqrt(jnp.full((1, TILE), squares[side]) / order + 1e-06)
            inverse = 1.0 / scale
            scales.append(jnp.exp(-0.25 * jnp.log(scale)))
            for tile in tiles:
                stat = new[side, :, columns(tile)]
                moment = jnp.where(eye(tile), stat + ridge, stat) * inverse
                put(base + M0, tile, moment)
                next_factor(base + F1, tile, moment)

        def both(first, second, use):
            for side in range(2):
                base = 9 * side
                for tile in tiles:
                    use(side, base, tile, multiply(base + first, base + second, tile))

        def into(slot):
            return lambda side, base, tile, value: put(base + slot, tile, value)

        def moment_and_factor(side, base, tile, value):
            put(base + M1, tile, value)
            next_factor(base + F2, tile, value)

        both(F1, F1, into(S))
        both(S, S, into(Q))
        both(Q, M0, moment_and_factor)
        both(F2, F2, into(S))
        both(F1, F2, lambda side, base, tile, value: put(base + X2, tile, value * scales[side]))
        both(S, S, into(Q))
        both(Q, M1, lambda side, base, tile, value: next_factor(base + F3, tile, value))
        both(X2, F3, into(X3))

    @pl.when(jnp.logical_not(due))
    def _():
        copies = [
            pltpu.make_async_copy(source, old.at[side], roots_sem.at[side])
            for side, source in enumerate((left_roots, right_roots))
        ]
        for copy in copies:
            copy.start()
        for side, copy in enumerate(copies):
            copy.wait()
            for tile in tiles:
                put(9 * side + X3, tile, old[side, :, columns(tile)])

    for tile in tiles:
        put(T, tile, multiply(X3, G, tile))
    for tile in tiles:
        g_ref[:, columns(tile)] = multiply(T, 9 + X3, tile)
    last = pltpu.make_async_copy(g_ref, precond, store_sem.at[2])
    last.start()
    for store in stores + [last]:
        store.wait()


def shards(inputs, out_grads, left_old, right_old, left_roots, right_roots, ages):
    order = left_old.shape[0]
    tokens_all = out_grads.shape[0] * lax.axis_size("dp")
    gradient = gather_product(inputs, out_grads, tokens_all ** (-0.5))
    anywhere = pl.BlockSpec(memory_space=pl.ANY)
    whole = jax.ShapeDtypeStruct((order, order), jnp.float32)
    return pl.pallas_call(
        roots_kernel,
        out_shape=(whole, whole, whole),
        in_specs=[
            pl.BlockSpec(memory_space=pltpu.SMEM),
            pl.BlockSpec(memory_space=pltpu.VMEM),
            anywhere, anywhere, anywhere, anywhere,
        ],
        out_specs=(anywhere, anywhere, anywhere),
        scratch_shapes=[
            pltpu.VMEM((2, order, order), jnp.float32),
            pltpu.VMEM((2, order, order), jnp.float32),
            pltpu.VMEM((SLOTS, order, order), jnp.bfloat16),
            pltpu.VMEM((SLOTS, order, order), jnp.bfloat16),
            pltpu.SemaphoreType.DMA((2,)),
            pltpu.SemaphoreType.DMA((3,)),
            pltpu.SemaphoreType.DMA((2,)),
        ],
        compiler_params=pltpu.CompilerParams(vmem_limit_bytes=50 * 1024 * 1024),
        name="roots",
    )(ages, gradient, left_old, right_old, left_roots, right_roots)


def solution(mesh):
    in_specs = (
        P("dp", "mp"),
        P("dp", "mp"),
        P("dp", "mp"),
        P("dp", "mp"),
        P("dp", "mp"),
        P("dp", "mp"),
        P(),
    )
    out_specs = (P("dp", "mp"), P("dp", "mp"), P("dp", "mp"))
    return jax.shard_map(shards, mesh=mesh, in_specs=in_specs, out_specs=out_specs, check_vma=False)
```

```python
import jax
import jax.numpy as jnp
from jax import lax
from jax.experimental import pallas as pl
from jax.experimental.pallas import tpu as pltpu
from jax.sharding import PartitionSpec as P

ITERS = 3
PERIOD = 100
NZ, NY, NX = 8, 4, 4
PARTS = 16
MESH = pl.DeviceIdType.MESH

decay_rate = 0.95
ridge = 0.001


UNITS = 4
SHIFT = (0, 6, 8, 14)
ORDER = (
    ("enter", 0), ("enter", 1), ("enter", 2), ("enter", 3), ("own", 0), ("own", 1), ("forward", 0),
    ("forward", 1), ("forward", 2), ("forward", 3), ("ring", 1, 0, -1), ("first", 0), ("first", 1),
    ("first", 2), ("first", 3), ("side", 0, 0, 1), ("ring", 1, 0, 1), ("near", 0, 1), ("near", 0, -1),
    ("own", 2), ("own", 3), ("near", 1, -1), ("near", 3, -1), ("ring", 1, 2, 1), ("side", 0, 0, -1),
    ("side", 2, 0, -1), ("ring", 1, 3, -1), ("ring", 1, 1, -1), ("side", 1, 0, -1), ("ring", 1, 3, 1),
    ("near", 2, 1), ("near", 2, -1), ("ring", 1, 1, 1), ("near", 1, 1), ("near", 3, 1),
    ("side", 2, 0, 1), ("side", 3, 0, -1), ("ring", 1, 2, -1), ("ring", 2, 0, 1), ("ring", 2, 0, -1),
    ("far", 0), ("side", 2, -1, -1), ("side", 1, 0, 1), ("ring", 2, 1, 1), ("far", 3), ("far", 2),
    ("ring", 2, 2, 1), ("far", 1), ("side", 0, -1, 1), ("ring", 2, 3, 1), ("ring", 2, 1, -1),
    ("side", 3, -1, 1), ("ring", 2, 3, -1), ("side", 0, 1, -1), ("side", 3, 1, 1), ("side", 3, 0, 1),
    ("side", 3, 1, -1), ("side", 0, 2, -1), ("ring", 2, 2, -1), ("side", 1, -1, -1), ("side", 1, 1, 1),
    ("side", 1, -1, 1), ("side", 3, -1, -1), ("side", 0, -1, -1), ("side", 0, 1, 1), ("ring", 3, 1, 1),
    ("ring", 3, 0, 1), ("side", 2, 1, 1), ("side", 1, 2, 1), ("side", 1, 1, -1), ("side", 2, -1, 1),
    ("ring", 3, 1, -1), ("side", 2, 2, -1), ("side", 0, 2, 1), ("side", 1, 2, -1), ("side", 2, 1, -1),
    ("ring", 3, 3, -1), ("ring", 3, 2, -1), ("side", 2, 2, 1), ("ring", 3, 3, 1), ("side", 3, 2, 1),
    ("ring", 3, 0, -1), ("side", 3, 2, -1), ("ring", 3, 2, 1), ("last", 1), ("last", 2), ("last", 3),
    ("last", 0),
)


def gather_kernel(
    scale, a_hbm, b_hbm, g_ref, abuf, bbuf, stage, load_sem, s_send, s_recv, t_send, t_recv,
    a_send, a_recv, b_send, b_recv,
):
    rows, width = a_hbm.shape
    count = rows // UNITS
    i = lax.axis_index("dp")
    k = lax.axis_index("mp")
    z, c = i // 2, i % 2
    y, x = k // NX, k % NX

    def place(dz=0, dy=0, dx=0, other=False):
        core = 1 - c if other else c
        return {
            "dp": ((z + dz + NZ) % NZ) * 2 + core,
            "mp": ((y + dy + NY) % NY) * NX + (x + dx + NX) % NX,
        }

    def near(u):
        return {"dp": i, "mp": (i + k + SHIFT[u]) % PARTS}

    def near_origin(u):
        return {"dp": i, "mp": (k - i - SHIFT[u] + 2 * PARTS) % PARTS}

    def token_block(u):
        return (k - i - SHIFT[u] + 2 * PARTS) % PARTS

    def partner(u):
        return {"dp": token_block(u), "mp": k}

    def stays(u):
        return (i + SHIFT[u]) % PARTS == 0

    def rows_of(u):
        return pl.ds(u * count, count)

    load = pltpu.make_async_copy(b_hbm, bbuf.at[i], load_sem.at[0])
    load.start()
    barrier = pltpu.get_barrier_semaphore()
    greeted = [
        place(dz=1), place(dz=-1), place(dy=1), place(dy=-1), place(dx=1), place(dx=-1),
        place(other=True),
    ]
    greeted += [device(u) for u in range(UNITS) for device in (near_origin, partner)]
    for device in greeted:
        pl.semaphore_signal(barrier, inc=1, device_id=device, device_id_type=MESH)
    pl.semaphore_wait(barrier, len(greeted))

    def first_hop(u, final, local):
        source = a_hbm.at[rows_of(u)]
        goal = abuf.at[i, rows_of(u)] if final else stage.at[u]
        arrived = (t_recv if final else s_recv).at[u]
        if local:
            return pltpu.make_async_copy(source, goal, arrived)
        return pltpu.make_async_remote_copy(
            src_ref=source,
            dst_ref=goal,
            send_sem=s_send.at[u],
            recv_sem=arrived,
            device_id=near(u),
            device_id_type=MESH,
        )

    def second_hop(u, slot):
        return pltpu.make_async_remote_copy(
            src_ref=stage.at[u],
            dst_ref=abuf.at[slot, rows_of(u)],
            send_sem=t_send.at[u],
            recv_sem=t_recv.at[u],
            device_id=partner(u),
            device_id_type=MESH,
        )

    def start_first_hop(u):
        for final in (False, True):
            for local in (False, True):

                @pl.when(((i == k) == final) & (stays(u) == local))
                def _():
                    first_hop(u, final, local).start()

    def forward(u):
        for local in (False, True):

            @pl.when((token_block(u) != i) & (stays(u) == local))
            def _():
                copy = first_hop(u, False, local)
                if local:
                    copy.wait()
                else:
                    copy.wait_recv()

        @pl.when(token_block(u) != i)
        def _():
            second_hop(u, i).start()

    def entered(u):
        @pl.when(token_block(u) != i)
        def _():
            second_hop(u, token_block(u)).wait_recv()

        for local in (False, True):

            @pl.when((token_block(u) == i) & (stays(u) == local))
            def _():
                copy = first_hop(u, True, local)
                if local:
                    copy.wait()
                else:
                    copy.wait_recv()

    def entry_sent(u):
        @pl.when(jnp.logical_not(stays(u)))
        def _():
            first_hop(u, False, False).wait_send()

        @pl.when(token_block(u) != i)
        def _():
            second_hop(u, i).wait_send()

    def a_copy(slot, u, index, device):
        window = abuf.at[slot, rows_of(u)]
        return pltpu.make_async_remote_copy(
            src_ref=window,
            dst_ref=window,
            send_sem=a_send.at[index],
            recv_sem=a_recv.at[slot, u],
            device_id=device,
            device_id_type=MESH,
        )

    def b_copy(slot, u, index, device):
        window = bbuf.at[slot] if u is None else bbuf.at[slot, rows_of(u)]
        return pltpu.make_async_remote_copy(
            src_ref=window,
            dst_ref=window,
            send_sem=b_send.at[index],
            recv_sem=b_recv.at[slot, u or 0],
            device_id=device,
            device_id_type=MESH,
        )

    pending = {a_copy: [], b_copy: []}

    def send(make, slot, u, device):
        copy = make(slot, u, len(pending[make]), device)
        pending[make].append(copy)
        copy.start()

    def arrive(make, slot, u):
        make(slot, u, 0, place(dx=1)).wait_recv()

    def z_slot(distance):
        return ((z + distance + NZ) % NZ) * 2 + c

    def ring_own(u):
        for step in (1, -1):
            send(b_copy, i, u, place(dz=step))

    def ring(distance, u, step):
        slot = z_slot(-step * distance)
        arrive(b_copy, slot, u)
        if distance < 3 or passes_on(u, step):
            send(b_copy, slot, u, place(dz=step))
        rung[distance, step] = rung.get((distance, step), 0) + 1
        if rung[distance, step] == UNITS:
            send(b_copy, slot, None, place(other=True))

    rung = {}

    def ring_last(u):
        arrive(b_copy, z_slot(4), u)

    def a_slot(u, p, s):
        dx, dy = (p, s) if u < 2 else (s, p)
        where = ((y + dy + NY) % NY) * NX + (x + dx + NX) % NX
        return (where - i - SHIFT[u] + 2 * PARTS) % PARTS

    def primary(u, step):
        return place(dx=step) if u < 2 else place(dy=step)

    def secondary(u, step):
        return place(dy=step) if u < 2 else place(dx=step)

    def passes_on(u, step):
        return u % 2 == (0 if step == 1 else 1)

    def first_step(u):
        entered(u)
        for step in (1, -1):
            send(a_copy, a_slot(u, 0, 0), u, primary(u, step))
        for step in (1, -1):
            send(a_copy, a_slot(u, 0, 0), u, secondary(u, step))

    def primary_near(u, step):
        slot = a_slot(u, -step, 0)
        arrive(a_copy, slot, u)
        if passes_on(u, step):
            send(a_copy, slot, u, primary(u, step))
        for side in (1, -1):
            send(a_copy, slot, u, secondary(u, side))

    def primary_far(u):
        slot = a_slot(u, 2, 0)
        arrive(a_copy, slot, u)
        for side in (1, -1):
            send(a_copy, slot, u, secondary(u, side))

    def secondary_near(u, p, step):
        slot = a_slot(u, p, -step)
        arrive(a_copy, slot, u)
        if passes_on(u, step):
            send(a_copy, slot, u, secondary(u, step))

    def columns_of(p, s):
        slots = [a_slot(u, p, s) for u in range(UNITS)]
        return [
            jnp.concatenate([buf[slot, rows_of(u)] for u, slot in enumerate(slots)], axis=0)
            for buf in (abuf, bbuf)
        ]

    def multiply(places):
        first, second = (
            jnp.concatenate(parts, axis=0) for parts in zip(*(columns_of(p, s) for p, s in places))
        )
        return lax.dot_general(
            first, second, (((0,), (0,)), ((), ())), preferred_element_type=jnp.float32
        )

    actions = {
        "enter": start_first_hop, "own": ring_own, "forward": forward, "first": first_step,
        "near": primary_near, "far": primary_far, "side": secondary_near, "ring": ring,
        "last": ring_last,
    }
    loaded = False
    for name, *where in ORDER:
        if name == "own" and not loaded:
            load.wait()
            send(b_copy, i, None, place(other=True))
            loaded = True
        actions[name](*where)
    send(b_copy, z_slot(4), None, place(other=True))
    for distance in range(NZ):
        arrive(b_copy, ((z + distance) % NZ) * 2 + 1 - c, None)
    g_ref[...] = multiply([(p, s) for s in (0, -1, 1) for p in (0, -1, 1, 2)])
    for p in (0, -1, 1, 2):
        for u in range(UNITS):
            arrive(a_copy, a_slot(u, p, 2), u)
    g_ref[...] = scale * (g_ref[...] + multiply([(p, 2) for p in (0, -1, 1, 2)]))

    for copies in pending.values():
        for copy in copies:
            copy.wait_send()
    for u in range(UNITS):
        entry_sent(u)


def gather_product(inputs, out_grads, scale):
    rows, width = inputs.shape
    columns = out_grads.shape[1]
    return pl.pallas_call(
        lambda *refs: gather_kernel(scale, *refs),
        out_shape=jax.ShapeDtypeStruct((width, columns), jnp.float32),
        in_specs=[pl.BlockSpec(memory_space=pltpu.HBM)] * 2,
        out_specs=pl.BlockSpec(memory_space=pltpu.VMEM),
        scratch_shapes=[
            pltpu.VMEM((PARTS, rows, width), jnp.bfloat16),
            pltpu.VMEM((PARTS, rows, columns), jnp.bfloat16),
            pltpu.VMEM((UNITS, rows // UNITS, width), jnp.bfloat16),
            pltpu.SemaphoreType.DMA((1,)),
            pltpu.SemaphoreType.DMA((UNITS,)),
            pltpu.SemaphoreType.DMA((UNITS,)),
            pltpu.SemaphoreType.DMA((UNITS,)),
            pltpu.SemaphoreType.DMA((UNITS,)),
            pltpu.SemaphoreType.DMA((60,)),
            pltpu.SemaphoreType.DMA((PARTS, UNITS)),
            pltpu.SemaphoreType.DMA((40,)),
            pltpu.SemaphoreType.DMA((PARTS, UNITS)),
        ],
        compiler_params=pltpu.CompilerParams(
            collective_id=0, has_side_effects=True, vmem_limit_bytes=24 * 1024 * 1024
        ),
        cost_estimate=pl.CostEstimate(
            flops=30_000_000_000, bytes_accessed=1 << 20, transcendentals=0
        ),
        name="gather_product",
    )(*(pltpu.with_memory_space_constraint(a, pltpu.HBM) for a in (inputs, out_grads)))


def split(value):
    high = value.astype(jnp.bfloat16)
    return high, (value - high.astype(jnp.float32)).astype(jnp.bfloat16)


def dot(first, second):
    return jnp.dot(first, second, preferred_element_type=jnp.float32)


SLOTS = 21
G, GT, T = 18, 19, 20
M0, F1, S, Q, M1, F2, X2, F3, X3 = range(9)
TILE = 256


def roots_kernel(
    ages, g_ref, left_old, right_old, left_roots, right_roots,
    precond, left_new, right_new, new, final, high, low, store_sem,
):
    order = g_ref.shape[0]
    due = ages[lax.axis_index("dp"), lax.axis_index("mp")] >= PERIOD
    tiles = range(order // TILE)
    spans = [pl.ds(tile * TILE, TILE) for tile in tiles]
    everything = pl.ds(0, order)
    blocks = [(0, 0), (0, 1), (1, 1)]
    diagonal = lax.broadcasted_iota(jnp.int32, (TILE, TILE), 0) == lax.broadcasted_iota(
        jnp.int32, (TILE, TILE), 1
    )

    def put(slot, rows, columns, value):
        high[slot, rows, columns], low[slot, rows, columns] = split(value)

    def multiply(first, second, rows, columns):
        right_high = high[second, :, columns]
        left_high = high[first, rows, :]
        return (
            dot(left_high, right_high)
            + dot(left_high, low[second, :, columns])
            + dot(low[first, rows, :], right_high)
        )

    def symmetric(first, second, use):
        for m, n in blocks:
            value = multiply(first, second, spans[m], spans[n])
            use(m, n, value)
            if m != n:
                use(n, m, value.T)

    def on_diagonal(m, n, value, shift):
        return jnp.where(diagonal, value + shift, value) if m == n else value

    for tile in tiles:
        part = g_ref[:, spans[tile]]
        put(G, everything, spans[tile], part)
        put(GT, spans[tile], everything, part.T)

    stores = []
    totals = []
    for side, (first, second, old, out) in enumerate(
        ((G, GT, left_old, left_new), (GT, G, right_old, right_new))
    ):
        squares = []

        def use(m, n, value):
            stat = decay_rate * old[spans[m], spans[n]] + value * (1.0 / order)
            new[side, spans[m], spans[n]] = stat
            ridged = on_diagonal(m, n, stat, ridge)
            squares.append(jnp.sum(ridged * ridged))

        symmetric(first, second, use)
        totals.append(sum(squares))
        store = pltpu.make_async_copy(new.at[side], out, store_sem.at[side])
        store.start()
        stores.append(store)

    def put_factor(slot, m, n, moment):
        put(slot, spans[m], spans[n], on_diagonal(m, n, -0.25 * moment, 1.25))

    @pl.when(due)
    def _():
        scales = []
        for side in range(2):
            base = 9 * side
            scale = jnp.sqrt(jnp.full((1, TILE), totals[side]) / order + 1e-06)
            inverse = 1.0 / scale
            scales.append(jnp.exp(-0.25 * jnp.log(scale)))
            for m in tiles:
                for n in tiles:
                    moment = on_diagonal(m, n, new[side, spans[m], spans[n]], ridge) * inverse
                    put(base + M0, spans[m], spans[n], moment)
                    put_factor(base + F1, m, n, moment)

        def both(first, second, use):
            for side in range(2):
                base = 9 * side
                symmetric(base + first, base + second, lambda m, n, v: use(side, base, m, n, v))

        def into(slot):
            return lambda side, base, m, n, v: put(base + slot, spans[m], spans[n], v)

        def moment_and_factor(side, base, m, n, value):
            put(base + M1, spans[m], spans[n], value)
            put_factor(base + F2, m, n, value)

        both(F1, F1, into(S))
        both(S, S, into(Q))
        both(Q, M0, moment_and_factor)
        both(F2, F2, into(S))
        both(
            F1, F2,
            lambda side, base, m, n, v: put(base + X2, spans[m], spans[n], v * scales[side]),
        )
        both(S, S, into(Q))
        both(Q, M1, lambda side, base, m, n, v: put_factor(base + F3, m, n, v))
        both(X2, F3, into(X3))

    @pl.when(jnp.logical_not(due))
    def _():
        for side, root in enumerate((left_roots, right_roots)):
            for span in spans:
                put(9 * side + X3, everything, span, root[:, span])

    for span in spans:
        put(T, everything, span, multiply(X3, G, everything, span))
    for tile, span in enumerate(spans):
        final[:, span] = multiply(T, 9 + X3, everything, span)
        store = pltpu.make_async_copy(
            final.at[:, span], precond.at[:, span], store_sem.at[2 + tile]
        )
        store.start()
        stores.append(store)
    for store in stores:
        store.wait()


def shards(inputs, out_grads, left_old, right_old, left_roots, right_roots, ages):
    order = left_old.shape[0]
    tokens_all = out_grads.shape[0] * lax.axis_size("dp")
    gradient = gather_product(inputs, out_grads, tokens_all ** (-0.5))
    outside = pl.BlockSpec(memory_space=pltpu.HBM)
    inside = pl.BlockSpec(memory_space=pltpu.VMEM)
    whole = jax.ShapeDtypeStruct((order, order), jnp.float32)
    return pl.pallas_call(
        roots_kernel,
        out_shape=(whole, whole, whole),
        in_specs=[
            pl.BlockSpec(memory_space=pltpu.SMEM),
            inside, inside, inside, inside, inside,
        ],
        out_specs=(outside, outside, outside),
        scratch_shapes=[
            pltpu.VMEM((2, order, order), jnp.float32),
            pltpu.VMEM((order, order), jnp.float32),
            pltpu.VMEM((SLOTS, order, order), jnp.bfloat16),
            pltpu.VMEM((SLOTS, order, order), jnp.bfloat16),
            pltpu.SemaphoreType.DMA((4,)),
        ],
        compiler_params=pltpu.CompilerParams(vmem_limit_bytes=40 * 1024 * 1024),
        name="roots",
    )(ages, gradient, left_old, right_old, left_roots, right_roots)


def solution(mesh):
    in_specs = (
        P("dp", "mp"),
        P("dp", "mp"),
        P("dp", "mp"),
        P("dp", "mp"),
        P("dp", "mp"),
        P("dp", "mp"),
        P(),
    )
    out_specs = (P("dp", "mp"), P("dp", "mp"), P("dp", "mp"))
    return jax.shard_map(shards, mesh=mesh, in_specs=in_specs, out_specs=out_specs, check_vma=False)
```

```python
import jax
import jax.numpy as jnp
from jax import lax
from jax.experimental import pallas as pl
from jax.experimental.pallas import tpu as pltpu
from jax.sharding import PartitionSpec as P

ITERS = 3
PERIOD = 100
NZ, NY, NX = 8, 4, 4
PARTS = 16
MESH = pl.DeviceIdType.MESH

decay_rate = 0.95
ridge = 0.001


UNITS = 4
SHIFT = (0, 6, 8, 14)
ORDER = (
    ("enter", 0), ("enter", 1), ("enter", 2), ("enter", 3), ("own", 0), ("cross", 0, 1), ("own", 1),
    ("own", 2), ("own", 3), ("forward", 0), ("forward", 1), ("ring", 1, 0, 1), ("ring", 1, 0, -1),
    ("forward", 2), ("forward", 3), ("ring", 1, 1, 1), ("ring", 1, 1, -1), ("first", 0),
    ("ring", 1, 2, 1), ("ring", 1, 2, -1), ("first", 1), ("ring", 1, 3, 1), ("cross", 1, 1),
    ("ring", 1, 3, -1), ("cross", 1, -1), ("first", 2), ("ring", 2, 0, 1), ("ring", 2, 0, -1),
    ("first", 3), ("near", 0, 1), ("near", 0, -1), ("side", 0, 0, 1), ("side", 0, 0, -1),
    ("near", 1, 1), ("near", 1, -1), ("ring", 2, 1, 1), ("ring", 2, 1, -1), ("side", 1, 0, 1),
    ("side", 1, 0, -1), ("near", 2, 1), ("near", 2, -1), ("ring", 2, 2, 1), ("ring", 2, 2, -1),
    ("side", 2, 0, 1), ("side", 2, 0, -1), ("near", 3, 1), ("near", 3, -1), ("side", 3, 0, 1),
    ("side", 3, 0, -1), ("ring", 2, 3, 1), ("cross", 2, 1), ("ring", 2, 3, -1), ("cross", 2, -1),
    ("far", 0), ("far", 1), ("ring", 3, 0, 1), ("ring", 3, 0, -1), ("far", 2), ("far", 3),
    ("side", 0, -1, 1), ("side", 0, -1, -1), ("ring", 3, 1, 1), ("ring", 3, 1, -1), ("side", 1, -1, 1),
    ("side", 1, -1, -1), ("side", 2, -1, 1), ("side", 2, -1, -1), ("ring", 3, 2, 1),
    ("ring", 3, 2, -1), ("side", 3, -1, 1), ("side", 3, -1, -1), ("side", 0, 1, 1), ("side", 0, 1, -1),
    ("side", 1, 1, 1), ("side", 1, 1, -1), ("ring", 3, 3, 1), ("cross", 3, 1), ("ring", 3, 3, -1),
    ("cross", 3, -1), ("side", 2, 1, 1), ("side", 2, 1, -1), ("side", 3, 1, 1), ("side", 3, 1, -1),
    ("side", 0, 2, 1), ("side", 0, 2, -1), ("side", 1, 2, 1), ("side", 1, 2, -1), ("side", 2, 2, 1),
    ("side", 2, 2, -1), ("side", 3, 2, 1), ("side", 3, 2, -1), ("last", 0), ("last", 1), ("last", 2),
    ("last", 3), ("cross", 4, 1),
)


def gather_kernel(
    scale, a_hbm, b_hbm, g_ref, abuf, bbuf, own, stage, load_sem, s_send, s_recv, t_send, t_recv,
    a_send, a_recv, b_send, b_recv,
):
    rows, width = a_hbm.shape
    count = rows // UNITS
    i = lax.axis_index("dp")
    k = lax.axis_index("mp")
    z, c = i // 2, i % 2
    y, x = k // NX, k % NX

    def place(dz=0, dy=0, dx=0, other=False):
        core = 1 - c if other else c
        return {
            "dp": ((z + dz + NZ) % NZ) * 2 + core,
            "mp": ((y + dy + NY) % NY) * NX + (x + dx + NX) % NX,
        }

    def near(u):
        return {"dp": i, "mp": (i + k + SHIFT[u]) % PARTS}

    def near_origin(u):
        return {"dp": i, "mp": (k - i - SHIFT[u] + 2 * PARTS) % PARTS}

    def token_block(u):
        return (k - i - SHIFT[u] + 2 * PARTS) % PARTS

    def partner(u):
        return {"dp": token_block(u), "mp": k}

    def stays(u):
        return (i + SHIFT[u]) % PARTS == 0

    def rows_of(u):
        return pl.ds(u * count, count)

    own_load = pltpu.make_async_copy(a_hbm, own, load_sem.at[1])
    own_load.start()
    load = pltpu.make_async_copy(b_hbm, bbuf.at[i], load_sem.at[0])
    load.start()
    barrier = pltpu.get_barrier_semaphore()
    greeted = [
        place(dz=1), place(dz=-1), place(dy=1), place(dy=-1), place(dx=1), place(dx=-1),
        place(other=True),
    ]
    greeted += [device(u) for u in range(UNITS) for device in (near_origin, partner)]
    for device in greeted:
        pl.semaphore_signal(barrier, inc=1, device_id=device, device_id_type=MESH)
    pl.semaphore_wait(barrier, len(greeted))
    own_load.wait()

    def first_hop(u, final, local):
        source = (a_hbm if local else own).at[rows_of(u)]
        goal = abuf.at[i, rows_of(u)] if final else stage.at[u]
        arrived = (t_recv if final else s_recv).at[u]
        if local:
            return pltpu.make_async_copy(source, goal, arrived)
        return pltpu.make_async_remote_copy(
            src_ref=source,
            dst_ref=goal,
            send_sem=s_send.at[u],
            recv_sem=arrived,
            device_id=near(u),
            device_id_type=MESH,
        )

    def second_hop(u, slot):
        return pltpu.make_async_remote_copy(
            src_ref=stage.at[u],
            dst_ref=abuf.at[slot, rows_of(u)],
            send_sem=t_send.at[u],
            recv_sem=t_recv.at[u],
            device_id=partner(u),
            device_id_type=MESH,
        )

    def start_first_hop(u):
        for final in (False, True):
            for local in (False, True):

                @pl.when(((i == k) == final) & (stays(u) == local))
                def _():
                    first_hop(u, final, local).start()

    def forward(u):
        for local in (False, True):

            @pl.when((token_block(u) != i) & (stays(u) == local))
            def _():
                copy = first_hop(u, False, local)
                if local:
                    copy.wait()
                else:
                    copy.wait_recv()

        @pl.when(token_block(u) != i)
        def _():
            second_hop(u, i).start()

    def entered(u):
        @pl.when(token_block(u) != i)
        def _():
            second_hop(u, token_block(u)).wait_recv()

        for local in (False, True):

            @pl.when((token_block(u) == i) & (stays(u) == local))
            def _():
                copy = first_hop(u, True, local)
                if local:
                    copy.wait()
                else:
                    copy.wait_recv()

    def entry_sent(u):
        @pl.when(jnp.logical_not(stays(u)))
        def _():
            first_hop(u, False, False).wait_send()

        @pl.when(token_block(u) != i)
        def _():
            second_hop(u, i).wait_send()

    def a_copy(slot, u, index, device):
        window = abuf.at[slot, rows_of(u)]
        return pltpu.make_async_remote_copy(
            src_ref=window,
            dst_ref=window,
            send_sem=a_send.at[index],
            recv_sem=a_recv.at[slot, u],
            device_id=device,
            device_id_type=MESH,
        )

    def b_copy(slot, u, index, device):
        window = bbuf.at[slot] if u is None else bbuf.at[slot, rows_of(u)]
        return pltpu.make_async_remote_copy(
            src_ref=window,
            dst_ref=window,
            send_sem=b_send.at[index],
            recv_sem=b_recv.at[slot, u or 0],
            device_id=device,
            device_id_type=MESH,
        )

    pending = {a_copy: [], b_copy: []}

    def send(make, slot, u, device):
        copy = make(slot, u, len(pending[make]), device)
        pending[make].append(copy)
        copy.start()

    def arrive(make, slot, u):
        make(slot, u, 0, place(dx=1)).wait_recv()

    def z_slot(distance):
        return ((z + distance + NZ) % NZ) * 2 + c

    def ring_own(u):
        for step in (1, -1):
            send(b_copy, i, u, place(dz=step))

    def ring(distance, u, step):
        slot = z_slot(-step * distance)
        arrive(b_copy, slot, u)
        if distance < 3 or passes_on(u, step):
            send(b_copy, slot, u, place(dz=step))

    def cross(distance, step):
        send(b_copy, z_slot(-step * distance), None, place(other=True))

    def ring_last(u):
        arrive(b_copy, z_slot(4), u)

    def a_slot(u, p, s):
        dx, dy = (p, s) if u < 2 else (s, p)
        where = ((y + dy + NY) % NY) * NX + (x + dx + NX) % NX
        return (where - i - SHIFT[u] + 2 * PARTS) % PARTS

    def primary(u, step):
        return place(dx=step) if u < 2 else place(dy=step)

    def secondary(u, step):
        return place(dy=step) if u < 2 else place(dx=step)

    def passes_on(u, step):
        return u % 2 == (0 if step == 1 else 1)

    def first_step(u):
        entered(u)
        for step in (1, -1):
            send(a_copy, a_slot(u, 0, 0), u, primary(u, step))
        for step in (1, -1):
            send(a_copy, a_slot(u, 0, 0), u, secondary(u, step))

    def primary_near(u, step):
        slot = a_slot(u, -step, 0)
        arrive(a_copy, slot, u)
        if passes_on(u, step):
            send(a_copy, slot, u, primary(u, step))
        for side in (1, -1):
            send(a_copy, slot, u, secondary(u, side))

    def primary_far(u):
        slot = a_slot(u, 2, 0)
        arrive(a_copy, slot, u)
        for side in (1, -1):
            send(a_copy, slot, u, secondary(u, side))

    def secondary_near(u, p, step):
        slot = a_slot(u, p, -step)
        arrive(a_copy, slot, u)
        if passes_on(u, step):
            send(a_copy, slot, u, secondary(u, step))

    def columns_of(p, s):
        slots = [a_slot(u, p, s) for u in range(UNITS)]
        return [
            jnp.concatenate([buf[slot, rows_of(u)] for u, slot in enumerate(slots)], axis=0)
            for buf in (abuf, bbuf)
        ]

    def multiply(places):
        first, second = (
            jnp.concatenate(parts, axis=0) for parts in zip(*(columns_of(p, s) for p, s in places))
        )
        return lax.dot_general(
            first, second, (((0,), (0,)), ((), ())), preferred_element_type=jnp.float32
        )

    actions = {
        "enter": start_first_hop, "own": ring_own, "forward": forward, "first": first_step,
        "near": primary_near, "far": primary_far, "side": secondary_near, "ring": ring,
        "last": ring_last, "cross": cross,
    }
    loaded = False
    for name, *where in ORDER:
        if name == "own" and not loaded:
            load.wait()
            loaded = True
        actions[name](*where)
    for distance in range(NZ):
        arrive(b_copy, ((z + distance) % NZ) * 2 + 1 - c, None)
    g_ref[...] = multiply([(p, s) for s in (0, -1, 1) for p in (0, -1, 1, 2)])
    for p in (0, -1, 1, 2):
        for u in range(UNITS):
            arrive(a_copy, a_slot(u, p, 2), u)
    g_ref[...] = scale * (g_ref[...] + multiply([(p, 2) for p in (0, -1, 1, 2)]))

    for copies in pending.values():
        for copy in copies:
            copy.wait_send()
    for u in range(UNITS):
        entry_sent(u)


def gather_product(inputs, out_grads, scale):
    rows, width = inputs.shape
    columns = out_grads.shape[1]
    return pl.pallas_call(
        lambda *refs: gather_kernel(scale, *refs),
        out_shape=jax.ShapeDtypeStruct((width, columns), jnp.float32),
        in_specs=[pl.BlockSpec(memory_space=pltpu.HBM)] * 2,
        out_specs=pl.BlockSpec(memory_space=pltpu.VMEM),
        scratch_shapes=[
            pltpu.VMEM((PARTS, rows, width), jnp.bfloat16),
            pltpu.VMEM((PARTS, rows, columns), jnp.bfloat16),
            pltpu.VMEM((rows, width), jnp.bfloat16),
            pltpu.VMEM((UNITS, rows // UNITS, width), jnp.bfloat16),
            pltpu.SemaphoreType.DMA((2,)),
            pltpu.SemaphoreType.DMA((UNITS,)),
            pltpu.SemaphoreType.DMA((UNITS,)),
            pltpu.SemaphoreType.DMA((UNITS,)),
            pltpu.SemaphoreType.DMA((UNITS,)),
            pltpu.SemaphoreType.DMA((60,)),
            pltpu.SemaphoreType.DMA((PARTS, UNITS)),
            pltpu.SemaphoreType.DMA((40,)),
            pltpu.SemaphoreType.DMA((PARTS, UNITS)),
        ],
        compiler_params=pltpu.CompilerParams(
            collective_id=0, has_side_effects=True, vmem_limit_bytes=24 * 1024 * 1024
        ),
        cost_estimate=pl.CostEstimate(
            flops=30_000_000_000, bytes_accessed=1 << 20, transcendentals=0
        ),
        name="gather_product",
    )(*(pltpu.with_memory_space_constraint(a, pltpu.HBM) for a in (inputs, out_grads)))


def split(value):
    high = value.astype(jnp.bfloat16)
    return high, (value - high.astype(jnp.float32)).astype(jnp.bfloat16)


def dot(first, second):
    return jnp.dot(first, second, preferred_element_type=jnp.float32)


SLOTS = 21
G, GT, T = 18, 19, 20
M0, F1, S, Q, M1, F2, X2, F3, X3 = range(9)
TILE = 256


def roots_kernel(
    ages, g_ref, left_old, right_old, left_roots, right_roots,
    precond, left_new, right_new, new, final, high, low, store_sem,
):
    order = g_ref.shape[0]
    due = ages[lax.axis_index("dp"), lax.axis_index("mp")] >= PERIOD
    tiles = range(order // TILE)
    spans = [pl.ds(tile * TILE, TILE) for tile in tiles]
    everything = pl.ds(0, order)
    blocks = [(0, 0), (0, 1), (1, 1)]
    diagonal = lax.broadcasted_iota(jnp.int32, (TILE, TILE), 0) == lax.broadcasted_iota(
        jnp.int32, (TILE, TILE), 1
    )

    def put(slot, rows, columns, value):
        high[slot, rows, columns], low[slot, rows, columns] = split(value)

    def multiply(first, second, rows, columns):
        right_high = high[second, :, columns]
        left_high = high[first, rows, :]
        return (
            dot(left_high, right_high)
            + dot(left_high, low[second, :, columns])
            + dot(low[first, rows, :], right_high)
        )

    def symmetric(first, second, use):
        for m, n in blocks:
            value = multiply(first, second, spans[m], spans[n])
            use(m, n, value)
            if m != n:
                use(n, m, value.T)

    def on_diagonal(m, n, value, shift):
        return jnp.where(diagonal, value + shift, value) if m == n else value

    for tile in tiles:
        part = g_ref[:, spans[tile]]
        put(G, everything, spans[tile], part)
        put(GT, spans[tile], everything, part.T)

    stores = []
    totals = []
    for side, (first, second, old, out) in enumerate(
        ((G, GT, left_old, left_new), (GT, G, right_old, right_new))
    ):
        squares = []

        def use(m, n, value):
            stat = decay_rate * old[spans[m], spans[n]] + value * (1.0 / order)
            new[side, spans[m], spans[n]] = stat
            ridged = on_diagonal(m, n, stat, ridge)
            squares.append(jnp.sum(ridged * ridged))

        symmetric(first, second, use)
        totals.append(sum(squares))
        store = pltpu.make_async_copy(new.at[side], out, store_sem.at[side])
        store.start()
        stores.append(store)

    def put_factor(slot, m, n, moment):
        put(slot, spans[m], spans[n], on_diagonal(m, n, -0.25 * moment, 1.25))

    @pl.when(due)
    def _():
        scales = []
        for side in range(2):
            base = 9 * side
            scale = jnp.sqrt(jnp.full((1, TILE), totals[side]) / order + 1e-06)
            inverse = 1.0 / scale
            scales.append(jnp.exp(-0.25 * jnp.log(scale)))
            for m in tiles:
                for n in tiles:
                    moment = on_diagonal(m, n, new[side, spans[m], spans[n]], ridge) * inverse
                    put(base + M0, spans[m], spans[n], moment)
                    put_factor(base + F1, m, n, moment)

        def both(first, second, use):
            for side in range(2):
                base = 9 * side
                symmetric(base + first, base + second, lambda m, n, v: use(side, base, m, n, v))

        def into(slot):
            return lambda side, base, m, n, v: put(base + slot, spans[m], spans[n], v)

        def moment_and_factor(side, base, m, n, value):
            put(base + M1, spans[m], spans[n], value)
            put_factor(base + F2, m, n, value)

        both(F1, F1, into(S))
        both(S, S, into(Q))
        both(Q, M0, moment_and_factor)
        both(F2, F2, into(S))
        both(
            F1, F2,
            lambda side, base, m, n, v: put(base + X2, spans[m], spans[n], v * scales[side]),
        )
        both(S, S, into(Q))
        both(Q, M1, lambda side, base, m, n, v: put_factor(base + F3, m, n, v))
        both(X2, F3, into(X3))

    @pl.when(jnp.logical_not(due))
    def _():
        for side, root in enumerate((left_roots, right_roots)):
            for span in spans:
                put(9 * side + X3, everything, span, root[:, span])

    for span in spans:
        put(T, everything, span, multiply(X3, G, everything, span))
    for tile, span in enumerate(spans):
        final[:, span] = multiply(T, 9 + X3, everything, span)
        store = pltpu.make_async_copy(
            final.at[:, span], precond.at[:, span], store_sem.at[2 + tile]
        )
        store.start()
        stores.append(store)
    for store in stores:
        store.wait()


def shards(inputs, out_grads, left_old, right_old, left_roots, right_roots, ages):
    order = left_old.shape[0]
    tokens_all = out_grads.shape[0] * lax.axis_size("dp")
    gradient = gather_product(inputs, out_grads, tokens_all ** (-0.5))
    outside = pl.BlockSpec(memory_space=pltpu.HBM)
    inside = pl.BlockSpec(memory_space=pltpu.VMEM)
    whole = jax.ShapeDtypeStruct((order, order), jnp.float32)
    return pl.pallas_call(
        roots_kernel,
        out_shape=(whole, whole, whole),
        in_specs=[
            pl.BlockSpec(memory_space=pltpu.SMEM),
            inside, inside, inside, inside, inside,
        ],
        out_specs=(outside, outside, outside),
        scratch_shapes=[
            pltpu.VMEM((2, order, order), jnp.float32),
            pltpu.VMEM((order, order), jnp.float32),
            pltpu.VMEM((SLOTS, order, order), jnp.bfloat16),
            pltpu.VMEM((SLOTS, order, order), jnp.bfloat16),
            pltpu.SemaphoreType.DMA((4,)),
        ],
        compiler_params=pltpu.CompilerParams(vmem_limit_bytes=40 * 1024 * 1024),
        name="roots",
    )(ages, gradient, left_old, right_old, left_roots, right_roots)


def solution(mesh):
    in_specs = (
        P("dp", "mp"),
        P("dp", "mp"),
        P("dp", "mp"),
        P("dp", "mp"),
        P("dp", "mp"),
        P("dp", "mp"),
        P(),
    )
    out_specs = (P("dp", "mp"), P("dp", "mp"), P("dp", "mp"))
    return jax.shard_map(shards, mesh=mesh, in_specs=in_specs, out_specs=out_specs, check_vma=False)
```

```python
import jax
import jax.numpy as jnp
from jax import lax
from jax.experimental import pallas as pl
from jax.experimental.pallas import tpu as pltpu
from jax.sharding import PartitionSpec as P

ITERS = 3
PERIOD = 100
NZ, NY, NX = 8, 4, 4
PARTS = 16
MESH = pl.DeviceIdType.MESH

decay_rate = 0.95
ridge = 0.001


UNITS = 4
SHIFT = (0, 6, 8, 14)
ORDER = (
    ("enter", 0), ("enter", 1), ("enter", 2), ("enter", 3), ("own", 0), ("cross", 0, 1), ("own", 1),
    ("own", 2), ("own", 3), ("forward", 0), ("forward", 1), ("ring", 1, 0, 1), ("ring", 1, 0, -1),
    ("forward", 2), ("forward", 3), ("ring", 1, 1, 1), ("ring", 1, 1, -1), ("first", 0),
    ("ring", 1, 2, 1), ("ring", 1, 2, -1), ("first", 1), ("ring", 1, 3, 1), ("cross", 1, 1),
    ("ring", 1, 3, -1), ("cross", 1, -1), ("first", 2), ("ring", 2, 0, 1), ("ring", 2, 0, -1),
    ("first", 3), ("near", 0, 1), ("near", 0, -1), ("side", 0, 0, 1), ("side", 0, 0, -1),
    ("near", 1, 1), ("near", 1, -1), ("ring", 2, 1, 1), ("ring", 2, 1, -1), ("side", 1, 0, 1),
    ("side", 1, 0, -1), ("near", 2, 1), ("near", 2, -1), ("ring", 2, 2, 1), ("ring", 2, 2, -1),
    ("side", 2, 0, 1), ("side", 2, 0, -1), ("near", 3, 1), ("near", 3, -1), ("side", 3, 0, 1),
    ("side", 3, 0, -1), ("ring", 2, 3, 1), ("cross", 2, 1), ("ring", 2, 3, -1), ("cross", 2, -1),
    ("far", 0), ("far", 1), ("ring", 3, 0, 1), ("ring", 3, 0, -1), ("far", 2), ("far", 3),
    ("side", 0, -1, 1), ("side", 0, -1, -1), ("ring", 3, 1, 1), ("ring", 3, 1, -1), ("side", 1, -1, 1),
    ("side", 1, -1, -1), ("side", 2, -1, 1), ("side", 2, -1, -1), ("ring", 3, 2, 1),
    ("ring", 3, 2, -1), ("side", 3, -1, 1), ("side", 3, -1, -1), ("side", 0, 1, 1), ("side", 0, 1, -1),
    ("side", 1, 1, 1), ("side", 1, 1, -1), ("ring", 3, 3, 1), ("cross", 3, 1), ("ring", 3, 3, -1),
    ("cross", 3, -1), ("side", 2, 1, 1), ("side", 2, 1, -1), ("side", 3, 1, 1), ("side", 3, 1, -1),
    ("side", 0, 2, 1), ("side", 0, 2, -1), ("side", 1, 2, 1), ("side", 1, 2, -1), ("side", 2, 2, 1),
    ("side", 2, 2, -1), ("side", 3, 2, 1), ("side", 3, 2, -1), ("last", 0), ("last", 1), ("last", 2),
    ("last", 3), ("cross", 4, 1),
)


def gather_kernel(
    scale, a_hbm, b_hbm, g_ref, abuf, bbuf, own, stage, load_sem, s_send, s_recv, t_send, t_recv,
    a_send, a_recv, b_send, b_recv,
):
    rows, width = a_hbm.shape
    count = rows // UNITS
    i = lax.axis_index("dp")
    k = lax.axis_index("mp")
    z, c = i // 2, i % 2
    y, x = k // NX, k % NX

    def place(dz=0, dy=0, dx=0, other=False):
        core = 1 - c if other else c
        return {
            "dp": ((z + dz + NZ) % NZ) * 2 + core,
            "mp": ((y + dy + NY) % NY) * NX + (x + dx + NX) % NX,
        }

    def near(u):
        return {"dp": i, "mp": (i + k + SHIFT[u]) % PARTS}

    def near_origin(u):
        return {"dp": i, "mp": (k - i - SHIFT[u] + 2 * PARTS) % PARTS}

    def token_block(u):
        return (k - i - SHIFT[u] + 2 * PARTS) % PARTS

    def partner(u):
        return {"dp": token_block(u), "mp": k}

    def stays(u):
        return (i + SHIFT[u]) % PARTS == 0

    def rows_of(u):
        return pl.ds(u * count, count)

    own_load = pltpu.make_async_copy(a_hbm, own, load_sem.at[1])
    own_load.start()
    load = pltpu.make_async_copy(b_hbm, bbuf.at[i], load_sem.at[0])
    load.start()
    barrier = pltpu.get_barrier_semaphore()
    greeted = [
        place(dz=1), place(dz=-1), place(dy=1), place(dy=-1), place(dx=1), place(dx=-1),
        place(other=True),
    ]
    greeted += [device(u) for u in range(UNITS) for device in (near_origin, partner)]
    for device in greeted:
        pl.semaphore_signal(barrier, inc=1, device_id=device, device_id_type=MESH)
    pl.semaphore_wait(barrier, len(greeted))
    own_load.wait()

    def first_hop(u, final, local):
        source = (a_hbm if local else own).at[rows_of(u)]
        goal = abuf.at[i, rows_of(u)] if final else stage.at[u]
        arrived = (t_recv if final else s_recv).at[u]
        if local:
            return pltpu.make_async_copy(source, goal, arrived)
        return pltpu.make_async_remote_copy(
            src_ref=source,
            dst_ref=goal,
            send_sem=s_send.at[u],
            recv_sem=arrived,
            device_id=near(u),
            device_id_type=MESH,
        )

    def second_hop(u, slot):
        return pltpu.make_async_remote_copy(
            src_ref=stage.at[u],
            dst_ref=abuf.at[slot, rows_of(u)],
            send_sem=t_send.at[u],
            recv_sem=t_recv.at[u],
            device_id=partner(u),
            device_id_type=MESH,
        )

    def start_first_hop(u):
        for final in (False, True):
            for local in (False, True):

                @pl.when(((i == k) == final) & (stays(u) == local))
                def _():
                    first_hop(u, final, local).start()

    def forward(u):
        for local in (False, True):

            @pl.when((token_block(u) != i) & (stays(u) == local))
            def _():
                copy = first_hop(u, False, local)
                if local:
                    copy.wait()
                else:
                    copy.wait_recv()

        @pl.when(token_block(u) != i)
        def _():
            second_hop(u, i).start()

    def entered(u):
        @pl.when(token_block(u) != i)
        def _():
            second_hop(u, token_block(u)).wait_recv()

        for local in (False, True):

            @pl.when((token_block(u) == i) & (stays(u) == local))
            def _():
                copy = first_hop(u, True, local)
                if local:
                    copy.wait()
                else:
                    copy.wait_recv()

    def entry_sent(u):
        @pl.when(jnp.logical_not(stays(u)))
        def _():
            first_hop(u, False, False).wait_send()

        @pl.when(token_block(u) != i)
        def _():
            second_hop(u, i).wait_send()

    def a_copy(slot, u, index, device):
        window = abuf.at[slot, rows_of(u)]
        return pltpu.make_async_remote_copy(
            src_ref=window,
            dst_ref=window,
            send_sem=a_send.at[index],
            recv_sem=a_recv.at[slot, u],
            device_id=device,
            device_id_type=MESH,
        )

    def b_copy(slot, u, index, device):
        window = bbuf.at[slot] if u is None else bbuf.at[slot, rows_of(u)]
        return pltpu.make_async_remote_copy(
            src_ref=window,
            dst_ref=window,
            send_sem=b_send.at[index],
            recv_sem=b_recv.at[slot, u or 0],
            device_id=device,
            device_id_type=MESH,
        )

    pending = {a_copy: [], b_copy: []}

    def send(make, slot, u, device):
        copy = make(slot, u, len(pending[make]), device)
        pending[make].append(copy)
        copy.start()

    def arrive(make, slot, u):
        make(slot, u, 0, place(dx=1)).wait_recv()

    def z_slot(distance):
        return ((z + distance + NZ) % NZ) * 2 + c

    def ring_own(u):
        for step in (1, -1):
            send(b_copy, i, u, place(dz=step))

    def ring(distance, u, step):
        slot = z_slot(-step * distance)
        arrive(b_copy, slot, u)
        if distance < 3 or passes_on(u, step):
            send(b_copy, slot, u, place(dz=step))

    def cross(distance, step):
        send(b_copy, z_slot(-step * distance), None, place(other=True))

    def ring_last(u):
        arrive(b_copy, z_slot(4), u)

    def a_slot(u, p, s):
        dx, dy = (p, s) if u < 2 else (s, p)
        where = ((y + dy + NY) % NY) * NX + (x + dx + NX) % NX
        return (where - i - SHIFT[u] + 2 * PARTS) % PARTS

    def primary(u, step):
        return place(dx=step) if u < 2 else place(dy=step)

    def secondary(u, step):
        return place(dy=step) if u < 2 else place(dx=step)

    def passes_on(u, step):
        return u % 2 == (0 if step == 1 else 1)

    def first_step(u):
        entered(u)
        for step in (1, -1):
            send(a_copy, a_slot(u, 0, 0), u, primary(u, step))
        for step in (1, -1):
            send(a_copy, a_slot(u, 0, 0), u, secondary(u, step))

    def primary_near(u, step):
        slot = a_slot(u, -step, 0)
        arrive(a_copy, slot, u)
        if passes_on(u, step):
            send(a_copy, slot, u, primary(u, step))
        for side in (1, -1):
            send(a_copy, slot, u, secondary(u, side))

    def primary_far(u):
        slot = a_slot(u, 2, 0)
        arrive(a_copy, slot, u)
        for side in (1, -1):
            send(a_copy, slot, u, secondary(u, side))

    def secondary_near(u, p, step):
        slot = a_slot(u, p, -step)
        arrive(a_copy, slot, u)
        if passes_on(u, step):
            send(a_copy, slot, u, secondary(u, step))

    def columns_of(p, s):
        slots = [a_slot(u, p, s) for u in range(UNITS)]
        return [
            jnp.concatenate([buf[slot, rows_of(u)] for u, slot in enumerate(slots)], axis=0)
            for buf in (abuf, bbuf)
        ]

    def multiply(places):
        first, second = (
            jnp.concatenate(parts, axis=0) for parts in zip(*(columns_of(p, s) for p, s in places))
        )
        return lax.dot_general(
            first, second, (((0,), (0,)), ((), ())), preferred_element_type=jnp.float32
        )

    actions = {
        "enter": start_first_hop, "own": ring_own, "forward": forward, "first": first_step,
        "near": primary_near, "far": primary_far, "side": secondary_near, "ring": ring,
        "last": ring_last, "cross": cross,
    }
    loaded = False
    for name, *where in ORDER:
        if name == "own" and not loaded:
            load.wait()
            loaded = True
        actions[name](*where)
    for distance in range(NZ):
        arrive(b_copy, ((z + distance) % NZ) * 2 + 1 - c, None)
    g_ref[...] = multiply([(p, s) for s in (0, -1, 1) for p in (0, -1, 1, 2)])
    for p in (0, -1, 1, 2):
        for u in range(UNITS):
            arrive(a_copy, a_slot(u, p, 2), u)
    g_ref[...] = scale * (g_ref[...] + multiply([(p, 2) for p in (0, -1, 1, 2)]))

    for copies in pending.values():
        for copy in copies:
            copy.wait_send()
    for u in range(UNITS):
        entry_sent(u)


def gather_product(inputs, out_grads, scale):
    rows, width = inputs.shape
    columns = out_grads.shape[1]
    return pl.pallas_call(
        lambda *refs: gather_kernel(scale, *refs),
        out_shape=jax.ShapeDtypeStruct((width, columns), jnp.float32),
        in_specs=[pl.BlockSpec(memory_space=pltpu.HBM)] * 2,
        out_specs=pl.BlockSpec(memory_space=pltpu.VMEM),
        scratch_shapes=[
            pltpu.VMEM((PARTS, rows, width), jnp.bfloat16),
            pltpu.VMEM((PARTS, rows, columns), jnp.bfloat16),
            pltpu.VMEM((rows, width), jnp.bfloat16),
            pltpu.VMEM((UNITS, rows // UNITS, width), jnp.bfloat16),
            pltpu.SemaphoreType.DMA((2,)),
            pltpu.SemaphoreType.DMA((UNITS,)),
            pltpu.SemaphoreType.DMA((UNITS,)),
            pltpu.SemaphoreType.DMA((UNITS,)),
            pltpu.SemaphoreType.DMA((UNITS,)),
            pltpu.SemaphoreType.DMA((60,)),
            pltpu.SemaphoreType.DMA((PARTS, UNITS)),
            pltpu.SemaphoreType.DMA((40,)),
            pltpu.SemaphoreType.DMA((PARTS, UNITS)),
        ],
        compiler_params=pltpu.CompilerParams(
            collective_id=0, has_side_effects=True, vmem_limit_bytes=24 * 1024 * 1024
        ),
        cost_estimate=pl.CostEstimate(
            flops=30_000_000_000, bytes_accessed=1 << 20, transcendentals=0
        ),
        name="gather_product",
    )(*(pltpu.with_memory_space_constraint(a, pltpu.HBM) for a in (inputs, out_grads)))


def split(value):
    high = value.astype(jnp.bfloat16)
    return high, (value - high.astype(jnp.float32)).astype(jnp.bfloat16)


def dot(first, second):
    return jnp.dot(first, second, preferred_element_type=jnp.float32)


SLOTS = 21
G, GT, T = 18, 19, 20
M0, F1, S, Q, M1, F2, X2, F3, X3 = range(9)
TILE = 256


def roots_kernel(
    ages, g_ref, left_old, right_old, left_roots, right_roots,
    precond, left_new, right_new, new, final, cross, high, low, store_sem,
):
    order = g_ref.shape[0]
    due = ages[lax.axis_index("dp"), lax.axis_index("mp")] >= PERIOD
    tiles = range(order // TILE)
    spans = [pl.ds(tile * TILE, TILE) for tile in tiles]
    everything = pl.ds(0, order)
    blocks = [(0, 0), (0, 1), (1, 1)]
    diagonal = lax.broadcasted_iota(jnp.int32, (TILE, TILE), 0) == lax.broadcasted_iota(
        jnp.int32, (TILE, TILE), 1
    )

    def put(slot, rows, columns, value):
        high[slot, rows, columns], low[slot, rows, columns] = split(value)

    def multiply(first, second, rows, columns):
        right_high = high[second, :, columns]
        left_high = high[first, rows, :]
        return (
            dot(left_high, right_high)
            + dot(left_high, low[second, :, columns])
            + dot(low[first, rows, :], right_high)
        )

    def symmetric(first, second, use):
        for m, n in blocks:
            value = multiply(first, second, spans[m], spans[n])
            use(m, n, value)
            if m != n:
                use(n, m, value.T)

    def square(first, second, use, side):
        for m in tiles:
            for n in tiles:
                cross[side, spans[m], spans[n]] = dot(
                    high[first, spans[m], :], low[second, :, spans[n]]
                )
        for m, n in blocks:
            value = dot(high[first, spans[m], :], high[second, :, spans[n]])
            other = cross[side, spans[n], spans[m]]
            value = value + (cross[side, spans[m], spans[n]] + other.T)
            use(m, n, value)
            if m != n:
                use(n, m, value.T)

    def on_diagonal(m, n, value, shift):
        return jnp.where(diagonal, value + shift, value) if m == n else value

    for tile in tiles:
        part = g_ref[:, spans[tile]]
        put(G, everything, spans[tile], part)
        put(GT, spans[tile], everything, part.T)

    stores = []
    totals = []
    for side, (first, second, old, out) in enumerate(
        ((G, GT, left_old, left_new), (GT, G, right_old, right_new))
    ):
        squares = []

        def use(m, n, value):
            stat = decay_rate * old[spans[m], spans[n]] + value * (1.0 / order)
            new[side, spans[m], spans[n]] = stat
            ridged = on_diagonal(m, n, stat, ridge)
            squares.append(jnp.sum(ridged * ridged))

        square(first, second, use, side)
        totals.append(sum(squares))
        store = pltpu.make_async_copy(new.at[side], out, store_sem.at[side])
        store.start()
        stores.append(store)

    def put_factor(slot, m, n, moment):
        put(slot, spans[m], spans[n], on_diagonal(m, n, -0.25 * moment, 1.25))

    @pl.when(due)
    def _():
        scales = []
        for side in range(2):
            base = 9 * side
            scale = jnp.sqrt(jnp.full((1, TILE), totals[side]) / order + 1e-06)
            inverse = 1.0 / scale
            scales.append(jnp.exp(-0.25 * jnp.log(scale)))
            for m in tiles:
                for n in tiles:
                    moment = on_diagonal(m, n, new[side, spans[m], spans[n]], ridge) * inverse
                    put(base + M0, spans[m], spans[n], moment)
                    put_factor(base + F1, m, n, moment)

        def both(first, second, use):
            for side in range(2):
                base = 9 * side

                def here(m, n, value):
                    use(side, base, m, n, value)

                if first == second:
                    square(base + first, base + second, here, side)
                else:
                    symmetric(base + first, base + second, here)

        def into(slot):
            return lambda side, base, m, n, v: put(base + slot, spans[m], spans[n], v)

        def moment_and_factor(side, base, m, n, value):
            put(base + M1, spans[m], spans[n], value)
            put_factor(base + F2, m, n, value)

        both(F1, F1, into(S))
        both(S, S, into(Q))
        both(Q, M0, moment_and_factor)
        both(F2, F2, into(S))
        both(
            F1, F2,
            lambda side, base, m, n, v: put(base + X2, spans[m], spans[n], v * scales[side]),
        )
        both(S, S, into(Q))
        both(Q, M1, lambda side, base, m, n, v: put_factor(base + F3, m, n, v))
        both(X2, F3, into(X3))

    @pl.when(jnp.logical_not(due))
    def _():
        for side, root in enumerate((left_roots, right_roots)):
            for span in spans:
                put(9 * side + X3, everything, span, root[:, span])

    for span in spans:
        put(T, everything, span, multiply(X3, G, everything, span))
    for tile, span in enumerate(spans):
        final[:, span] = multiply(T, 9 + X3, everything, span)
        store = pltpu.make_async_copy(
            final.at[:, span], precond.at[:, span], store_sem.at[2 + tile]
        )
        store.start()
        stores.append(store)
    for store in stores:
        store.wait()


def shards(inputs, out_grads, left_old, right_old, left_roots, right_roots, ages):
    order = left_old.shape[0]
    tokens_all = out_grads.shape[0] * lax.axis_size("dp")
    gradient = gather_product(inputs, out_grads, tokens_all ** (-0.5))
    outside = pl.BlockSpec(memory_space=pltpu.HBM)
    inside = pl.BlockSpec(memory_space=pltpu.VMEM)
    whole = jax.ShapeDtypeStruct((order, order), jnp.float32)
    return pl.pallas_call(
        roots_kernel,
        out_shape=(whole, whole, whole),
        in_specs=[
            pl.BlockSpec(memory_space=pltpu.SMEM),
            inside, inside, inside, inside, inside,
        ],
        out_specs=(outside, outside, outside),
        scratch_shapes=[
            pltpu.VMEM((2, order, order), jnp.float32),
            pltpu.VMEM((order, order), jnp.float32),
            pltpu.VMEM((2, order, order), jnp.float32),
            pltpu.VMEM((SLOTS, order, order), jnp.bfloat16),
            pltpu.VMEM((SLOTS, order, order), jnp.bfloat16),
            pltpu.SemaphoreType.DMA((4,)),
        ],
        compiler_params=pltpu.CompilerParams(vmem_limit_bytes=40 * 1024 * 1024),
        name="roots",
    )(ages, gradient, left_old, right_old, left_roots, right_roots)


def solution(mesh):
    in_specs = (
        P("dp", "mp"),
        P("dp", "mp"),
        P("dp", "mp"),
        P("dp", "mp"),
        P("dp", "mp"),
        P("dp", "mp"),
        P(),
    )
    out_specs = (P("dp", "mp"), P("dp", "mp"), P("dp", "mp"))
    return jax.shard_map(shards, mesh=mesh, in_specs=in_specs, out_specs=out_specs, check_vma=False)
```
